32 devices in a mesh: dp: 2 (over x), tp: 4 (over z), sp: 4 (over y, core).
Axes of the slice: x: 2, y: 2, z: 4, core: 2. Of those that a mesh axis runs over, the one named last changes fastest.
Arguments:
- encoded: bfloat16 [128, 512, 768], P('dp', 'sp'), parts along dimension 0
- enc_gain: float32 [768], replicated
- enc_bias: float32 [768], replicated
- probe: float32 [768], replicated
- w_query: bfloat16 [768, 12, 64], P(None, 'tp')
- b_query: float32 [12, 64], P('tp')
- w_key: bfloat16 [768, 12, 64], P(None, 'tp')
- w_value: bfloat16 [768, 12, 64], P(None, 'tp')
- b_value: float32 [12, 64], P('tp')
- w_out: bfloat16 [12, 64, 768], P('tp')
- b_out: float32 [768], replicated
- head_gain: float32 [768], replicated
- head_bias: float32 [768], replicated
- w_up: bfloat16 [768, 3072], P(None, 'tp')
- b_up: float32 [3072], P('tp')
- w_down: bfloat16 [3072, 768], P('tp')
- b_down: float32 [768], replicated
- out_grad: bfloat16 [128, 768], P('dp'), parts along dimension 0
Outputs:
- output 1: bfloat16 [128, 768], P('dp'), parts along dimension 0
- output 2: bfloat16 [128, 512, 768], P('dp', 'sp'), parts along dimension 0
- output 3: float32 [1536], P('dp'), parts along dimension 0
- output 4: float32 [1536, 12, 64], P('dp', 'tp'), parts along dimension 0
- output 5: float32 [1536, 12, 64], P('dp', 'tp'), parts along dimension 0
- output 6: float32 [1536, 12, 64], P('dp', 'tp'), parts along dimension 0
- output 7: float32 [24, 64, 768], P(('dp', 'tp')), parts along dimension 0
- output 8: float32 [1536, 3072], P('dp', 'tp'), parts along dimension 0
- output 9: float32 [6144, 768], P(('dp', 'tp')), parts along dimension 0
There are 2 independent parts. The reference program is written for one: setup_inputs(seed, part) draws one part's arguments, and reference() takes and returns one part's arrays. A program takes and returns all parts, laid end to end along the dimension named above; an argument that names none is the same for every part.
All inputs are finite; a program needn't handle non-finite values.
Results may differ from the reference program's by a relative error of at most 0.0186479.
Values sent between devices are 32-bit elements.
A program may use at most 1 GiB of HBM per device.

```python
import jax
import jax.numpy as jnp
from jax import lax

IMAGES = 64
TOKENS = 512
MODEL_WIDTH = 768
NUM_HEADS = 12
MLP_WIDTH = 3072
HEAD_DIM = MODEL_WIDTH // NUM_HEADS
NORM_EPS = 1e-6


def normal_weight(key_in, shape_in, fan_in):
    return (jax.random.normal(key_in, shape_in, jnp.float32) * fan_in ** -0.5).astype(jnp.bfloat16)


def normal_vector(key_in, shape_in, center, spread):
    return center + spread * jax.random.normal(key_in, shape_in, jnp.float32)


def setup_inputs(seed: int = 0, part: int = 0) -> dict:
    base_key = jax.random.key(seed)
    shared_keys = jax.random.split(base_key, 16)
    part_keys = jax.random.split(jax.random.fold_in(base_key, part), 4)
    head_shape = (MODEL_WIDTH, NUM_HEADS, HEAD_DIM)
    positions = jnp.linspace(-1.5, 1.5, TOKENS, dtype=jnp.float32)
    token_noise = jax.random.normal(part_keys[0], (IMAGES, TOKENS, MODEL_WIDTH), jnp.float32)
    common = jax.random.normal(part_keys[1], (IMAGES, 1, MODEL_WIDTH), jnp.float32)
    trend_dir = jax.random.normal(part_keys[2], (IMAGES, 1, MODEL_WIDTH), jnp.float32)
    encoded = (token_noise + common + positions[None, :, None] * trend_dir).astype(jnp.bfloat16)
    out_grad = jax.random.normal(part_keys[3], (IMAGES, MODEL_WIDTH), jnp.float32).astype(jnp.bfloat16)
    return {
        'encoded': encoded,
        'enc_gain': normal_vector(shared_keys[0], (MODEL_WIDTH,), 1.0, 0.3),
        'enc_bias': normal_vector(shared_keys[1], (MODEL_WIDTH,), 0.0, 0.5),
        'probe': normal_vector(shared_keys[2], (MODEL_WIDTH,), 0.0, 1.0),
        'w_query': normal_weight(shared_keys[3], head_shape, MODEL_WIDTH),
        'b_query': normal_vector(shared_keys[4], (NUM_HEADS, HEAD_DIM), 0.0, 0.5),
        'w_key': normal_weight(shared_keys[5], head_shape, MODEL_WIDTH),
        'w_value': normal_weight(shared_keys[6], head_shape, MODEL_WIDTH),
        'b_value': normal_vector(shared_keys[7], (NUM_HEADS, HEAD_DIM), 0.0, 0.5),
        'w_out': normal_weight(shared_keys[8], (NUM_HEADS, HEAD_DIM, MODEL_WIDTH), MODEL_WIDTH),
        'b_out': normal_vector(shared_keys[9], (MODEL_WIDTH,), 0.0, 0.5),
        'head_gain': normal_vector(shared_keys[10], (MODEL_WIDTH,), 1.0, 0.3),
        'head_bias': normal_vector(shared_keys[11], (MODEL_WIDTH,), 0.0, 0.5),
        'w_up': normal_weight(shared_keys[12], (MODEL_WIDTH, MLP_WIDTH), MODEL_WIDTH),
        'b_up': normal_vector(shared_keys[13], (MLP_WIDTH,), 0.0, 0.5),
        'w_down': normal_weight(shared_keys[14], (MLP_WIDTH, MODEL_WIDTH), MLP_WIDTH),
        'b_down': normal_vector(shared_keys[15], (MODEL_WIDTH,), 0.0, 0.5),
        'out_grad': out_grad,
    }


def layer_norm(rows_in, norm_gain, norm_bias):
    row_mean = jnp.mean(rows_in, axis=-1, keepdims=True)
    centred = rows_in - row_mean
    inv_std = lax.rsqrt(jnp.mean(centred * centred, axis=-1, keepdims=True) + NORM_EPS)
    return centred * inv_std * norm_gain + norm_bias


def keep_exact(array_in):
    return array_in


def store_bf16(array_in):
    return array_in.astype(jnp.bfloat16).astype(jnp.float32)


def head_forward(store, encoded, enc_gain, enc_bias, probe, w_query, b_query, w_key, w_value, b_value, w_out, b_out, head_gain, head_bias, w_up, b_up, w_down, b_down):
    normed = store(layer_norm(encoded, enc_gain, enc_bias))
    query_heads = store(jnp.einsum('w,whd->hd', store(probe), w_query) + b_query)
    key_heads = store(jnp.einsum('bnw,whd->bnhd', normed, w_key))
    value_heads = store(jnp.einsum('bnw,whd->bnhd', normed, w_value) + b_value)
    scores = jnp.einsum('bnhd,hd->bhn', key_heads, query_heads) * HEAD_DIM ** -0.5
    weights = jax.nn.softmax(scores, axis=-1)
    pooled_heads = store(jnp.einsum('bhn,bnhd->bhd', weights, value_heads))
    attn_out = jnp.einsum('bhd,hdw->bw', pooled_heads, w_out) + b_out
    normed_out = store(layer_norm(attn_out, head_gain, head_bias))
    hidden = store(jax.nn.gelu(jnp.dot(normed_out, w_up) + b_up, approximate=True))
    return attn_out + jnp.dot(hidden, w_down) + b_down


def reference(encoded, enc_gain, enc_bias, probe, w_query, b_query, w_key, w_value, b_value, w_out, b_out, head_gain, head_bias, w_up, b_up, w_down, b_down, out_grad):
    exact_args = [array_in.astype(jnp.float32) for array_in in (encoded, enc_gain, enc_bias, probe, w_query, b_query, w_key, w_value, b_value, w_out, b_out, head_gain, head_bias, w_up, b_up, w_down, b_down)]
    pooled = head_forward(store_bf16, *exact_args).astype(jnp.bfloat16)

    def grad_target(enc_in, probe_in, query_in, key_in, value_in, out_in, up_in, down_in):
        return head_forward(keep_exact, enc_in, exact_args[1], exact_args[2], probe_in, query_in, exact_args[5], key_in, value_in, exact_args[8], out_in, exact_args[10], exact_args[11], exact_args[12], up_in, exact_args[14], down_in, exact_args[16])

    pull_back = jax.vjp(grad_target, exact_args[0], exact_args[3], exact_args[4], exact_args[6], exact_args[7], exact_args[9], exact_args[13], exact_args[15])[1]
    grad_list = pull_back(out_grad.astype(jnp.float32))
    return (pooled, grad_list[0].astype(jnp.bfloat16), grad_list[1], grad_list[2], grad_list[3], grad_list[4], grad_list[5], grad_list[6], grad_list[7])
```

```python
import functools
import jax
import jax.numpy as jnp
from jax import lax
from jax.experimental import pallas as pl
from jax.experimental.pallas import tpu as pltpu
from jax.sharding import PartitionSpec as P

NORM_EPS = 1e-6
IN_SPECS = (P('dp', 'sp', None), P(), P(), P(), P(None, 'tp', None), P('tp', None), P(None, 'tp', None), P(None, 'tp', None), P('tp', None), P('tp', None, None), P(), P(), P(), P(None, 'tp'), P('tp'), P('tp', None), P(), P('dp', None))
OUT_SPECS = (P('dp', None), P('dp', 'sp', None), P('dp'), P('dp', 'tp', None), P('dp', 'tp', None), P('dp', 'tp', None), P(('dp', 'tp'), None, None), P('dp', 'tp'), P(('dp', 'tp'), None))
F32, BF16 = jnp.float32, jnp.bfloat16
MESH = pl.DeviceIdType.MESH
IMGS, TOK, WIDTH, HD, HEADS, TP, SP = 64, 128, 768, 64, 3, 4, 4
ROWS = IMGS * TOK
HDS = HEADS * HD
GROUP = IMGS // SP
SLOT = 8
SLOTS = TP * SLOT
QUARTER = HDS // 4
SCALE = HD ** -0.5


def dot(a, b, dims):
    return lax.dot_general(a, b, (dims, ((), ())), preferred_element_type=F32)


nn = functools.partial(dot, dims=((1,), (0,)))
nt = functools.partial(dot, dims=((1,), (1,)))
tn = functools.partial(dot, dims=((0,), (0,)))


def hi_lo(a):
    hi = a.astype(BF16).astype(F32)
    return jnp.concatenate([hi, a - hi], axis=0).astype(BF16)


def fold(a):
    half = a.shape[0] // 2
    return a[:half] + a[half:]


def row_mean(a):
    return jnp.mean(a, axis=-1, keepdims=True)


def iota(shape, axis):
    return lax.broadcasted_iota(jnp.int32, shape, axis)


def middle_kernel(x_hbm, gain_1d, bias_1d, probe_1d, wq, wk, wv, wo, bq_ref, bv_ref, bout_1d, hgain_1d, hbias_1d, bup_1d, bdown_1d, wup_hbm, wdown_hbm, og,
                  pooled_o, a_o, z_o, uc_o, c2_o, y_o, hid_o, gpre_o, ga_o, o_o, go_o, hb_o, r_o, gq_o, q_o, gp_o,
                  hx, wup, wdown, u_all, s_ref, e_ref, ml, f_ref, fo_ref, d_ref, hb, hbrx, hbg, arx, att_all, o_all,
                  gnp, gnrx, plp, plrx, pl_all, go_all, ga_all, wv_all, zl, z_ref, rrx, gprx, lsem, ssem, rsem):
    dp, t, s = lax.axis_index('dp'), lax.axis_index('tp'), lax.axis_index('sp')
    s1 = s + 1 - 2 * lax.rem(s, 2)
    s2 = lax.rem(s + 2, 4)
    s3 = lax.rem(s1 + 2, 4)
    sps = (s, s1, s2, s3)
    tps = tuple(lax.rem(t + k, 4) for k in range(4))
    mine = pl.ds(pl.multiple_of(s * GROUP, GROUP), GROUP)
    started = []
    index = iter(range(128))

    def remote(src, dst, sem, device):
        copy = pltpu.make_async_remote_copy(src_ref=src, dst_ref=dst, send_sem=ssem.at[sem], recv_sem=rsem.at[sem], device_id=device, device_id_type=MESH)
        copy.start()
        started.append(copy)
        return copy

    def to_tp(src, dst):
        return [remote(src, dst, next(index), (dp, tps[k], s)) for k in (2, 1, 3)]

    def to_sp(src, dst):
        return [remote(src, dst, next(index), (dp, t, sps[d])) for d in (3, 2, 1)]

    def arrive(copies):
        for copy in copies:
            copy.wait_recv()

    chunk = ROWS // 8
    x_copies = [pltpu.make_async_copy(x_hbm.at[pl.ds(i * chunk, chunk)], hx.at[pl.ds(i * chunk, chunk)], lsem.at[i]) for i in range(8)]
    x_copies += [pltpu.make_async_copy(wup_hbm, wup, lsem.at[8]), pltpu.make_async_copy(wdown_hbm, wdown, lsem.at[9])]
    for copy in x_copies:
        copy.start()

    o_all[...] = jnp.zeros_like(o_all)
    go_all[...] = jnp.zeros_like(go_all)
    gprx[...] = jnp.zeros_like(gprx)
    barrier = pltpu.get_barrier_semaphore()
    peers = [(dp, tps[k], sps[d]) for k in range(4) for d in range(4) if (k, d) != (0, 0)]
    peers += [(1 - dp, t, s), (1 - dp, t, s1)]
    for peer in peers:
        pl.semaphore_signal(barrier, inc=1, device_id=peer, device_id_type=MESH)

    gain, bias, probe, bout, hgain, hbias, bup, bdown = [v[...].reshape(1, WIDTH) for v in (gain_1d, bias_1d, probe_1d, bout_1d, hgain_1d, hbias_1d, bup_1d, bdown_1d)]
    bq, bv = [jnp.concatenate([v[h:h + 1] for h in range(HEADS)], axis=1) for v in (bq_ref, bv_ref)]
    probe_rows = jnp.broadcast_to(probe, (16, WIDTH)).astype(BF16)
    query = (nt(probe_rows, wq[...]) + bq).astype(BF16).astype(F32)
    diag = iota((SLOT, HDS), 0) == iota((SLOT, HDS), 1) // HD
    query_diag = jnp.where(diag, query[:SLOT], 0.0)
    u_all[t] = fold(nn(hi_lo(query_diag), wk[...]))
    wv_all[t] = wv[...].astype(F32)
    q_o[...] = jnp.zeros_like(q_o)
    gq_o[...] = jnp.zeros_like(gq_o)
    q_o[:, 0:HDS] = query[:SLOT]

    pl.semaphore_wait(barrier, len(peers))
    u_copies = to_tp(u_all.at[t], u_all.at[t])
    part = lax.rem(s, 2) + 2 * dp
    part_rows = pl.ds(pl.multiple_of(part * QUARTER, 16), QUARTER)
    wv_copies = to_tp(wv_all.at[t, part_rows], wv_all.at[t, part_rows])

    step_rows = 256
    gain_row, bias_row = gain, bias

    def norm_step(i):
        rows = pl.ds(pl.multiple_of(i * step_rows, step_rows), step_rows)
        x = hx[rows].astype(F32)
        centred = x - row_mean(x)
        inv = lax.rsqrt(row_mean(centred * centred) + NORM_EPS)
        hx[rows] = (centred * inv * gain_row + bias_row).astype(BF16)

    for c in range(8):
        x_copies[c].wait()
        pl.loop(c * chunk // step_rows, (c + 1) * chunk // step_rows)(norm_step)

    arrive(u_copies)
    u = u_all[...].reshape(SLOTS, WIDTH)
    u_split = hi_lo(u)
    lane = iota((SLOTS, TOK), 1)
    wide = 512

    def score_step(i, carry):
        m_all, l_all = carry
        rows = pl.ds(pl.multiple_of(i * wide, wide), wide)
        raw = fold(nt(u_split, hx[rows]))
        s_ref[:, :, rows] = raw.reshape(TP, SLOT, wide)
        for j in range(wide // TOK):
            score = raw[:, j * TOK:(j + 1) * TOK] * SCALE
            top = jnp.max(score, axis=1, keepdims=True)
            e = jnp.exp(score - top)
            total = jnp.sum(e, axis=1, keepdims=True)
            e_ref[:, :, pl.ds(pl.multiple_of(i * wide + j * TOK, TOK), TOK)] = e.reshape(TP, SLOT, TOK)
            here = lane == i * (wide // TOK) + j
            m_all = jnp.where(here, top, m_all)
            l_all = jnp.where(here, total, l_all)
        return m_all, l_all

    m_own, l_own = lax.fori_loop(0, ROWS // wide, score_step, (jnp.zeros((SLOTS, TOK), F32), jnp.ones((SLOTS, TOK), F32)))
    ml[s, 0:SLOTS] = m_own
    ml[s, SLOTS:] = l_own
    ml_copies = to_sp(ml.at[s], ml.at[s])

    def pooled_step(b, row_base):
        image = row_base + b
        e_own = e_ref[t, :, pl.ds(pl.multiple_of(image * TOK, TOK), TOK)]
        result = fold(nn(hi_lo(e_own), hx[pl.ds(pl.multiple_of(image * TOK, TOK), TOK)]))
        for h in range(HEADS):
            hb[h, pl.ds(image, 1), :] = result[h:h + 1]

    hb_copies = []
    for d in (3, 2, 1, 0):
        base = pl.multiple_of(sps[d] * GROUP, GROUP)
        pl.loop(0, GROUP, unroll=4)(functools.partial(pooled_step, row_base=base))
        if d == 3:
            arrive(ml_copies)
            tops = [ml[k, 0:SLOTS] for k in range(SP)]
            top = functools.reduce(jnp.maximum, tops)
            total = sum(ml[k, SLOTS:] * jnp.exp(tops[k] - top) for k in range(SP))
            f_ref[...] = (jnp.exp(m_own - top) / total).reshape(TP, SLOT, TOK)
            fo_ref[...] = f_ref[t].T
        group = pl.ds(base, GROUP)
        for h in range(HEADS):
            hb[h, group, :] = hb[h, group, :] * fo_ref[group, h:h + 1]
        if d:
            hb_copies.append(remote(hb.at[:, group], hbrx.at[s], next(index), (dp, t, sps[d])))

    arrive(wv_copies)
    forward_copies = []
    for k in (2, 1, 3):
        block = wv_all.at[tps[(4 - k) % 4], part_rows]
        for device in ((dp, t, s1), (1 - dp, t, s), (1 - dp, t, s1)):
            forward_copies.append(remote(block, block, next(index), device))

    arrive(hb_copies)
    lane_head = iota((GROUP, HDS), 1) // HD
    o = jnp.zeros((GROUP, HDS), F32)
    for h in range(HEADS):
        hsum = hb[h, mine, :] + hbrx[s1, h] + hbrx[s2, h] + hbrx[s3, h]
        hbg[h, mine, :] = hsum
        o = jnp.where(lane_head == h, fold(nt(hi_lo(hsum), wv[...])), o)
    o_plain = o
    o = o + bv
    o_all[mine, 0:HDS] = o
    arx[t] = nn(o.astype(BF16), wo[...])
    att_copies = to_tp(arx.at[t], arx.at[t])
    x_copies[8].wait()
    x_copies[9].wait()
    grad_hidden = nt(og[...], wdown[...])
    arrive(att_copies)
    att_all[mine, :] = arx[0] + arx[1] + arx[2] + arx[3] + bout
    att_copies = to_sp(att_all.at[mine], att_all.at[mine])
    o_copies = to_sp(o_all.at[mine], o_all.at[mine])
    arrive(att_copies)

    att = att_all[...]
    centred = att - row_mean(att)
    inv = lax.rsqrt(row_mean(centred * centred) + NORM_EPS)
    y = (centred * inv * hgain + hbias).astype(BF16)
    y_o[...] = y
    pre = nn(y, wup[...]) + bup
    square = pre * pre
    tanh = jnp.tanh((2 / jnp.pi) ** 0.5 * (pre + 0.044715 * (square * pre)))
    hid = (0.5 * pre * (1.0 + tanh)).astype(BF16)
    slope = 0.5 * (1.0 + tanh) + 0.5 * pre * (1.0 - tanh * tanh) * ((2 / jnp.pi) ** 0.5 * (1.0 + 3 * 0.044715 * square))
    gpre = (grad_hidden * slope).astype(BF16)
    gpre_o[...] = gpre
    hid_o[...] = hid
    gnp[...] = nt(gpre, wup[...])
    gnrx[t] = gnp[mine, :]
    gn_copies = to_tp(gnrx.at[t], gnrx.at[t])
    plp[...] = nn(hid, wdown[...])
    plrx[t] = plp[mine, :]
    pl_copies = to_tp(plrx.at[t], plrx.at[t])
    arrive(gn_copies)
    grad_y = (gnrx[0] + gnrx[1] + gnrx[2] + gnrx[3]) * hgain
    att16 = att_all[mine, :]
    centred = att16 - row_mean(att16)
    inv = lax.rsqrt(row_mean(centred * centred) + NORM_EPS)
    unit = centred * inv
    grad_att = og[mine, :].astype(F32) + inv * (grad_y - row_mean(grad_y) - unit * row_mean(grad_y * unit))
    go = nt(grad_att.astype(BF16), wo[...]).astype(BF16).astype(F32)
    tail_lane = iota((GROUP, HD), 1)
    tail = jnp.zeros((GROUP, HD), F32)
    for h in range(HEADS):
        delta = jnp.sum(jnp.where(lane_head == h, go * o_plain, 0.0), axis=1, keepdims=True)
        tail = jnp.where(tail_lane == h, delta, tail)
    go_all[t, mine, 0:HDS] = go
    go_all[t, mine, HDS:] = tail
    go_copies = to_tp(go_all.at[t, mine], go_all.at[t, mine])
    ga_all[mine, :] = grad_att
    arrive(go_copies)
    go_copies = to_sp(go_all.at[:, mine], go_all.at[:, mine])
    ga_copies = to_sp(ga_all.at[mine], ga_all.at[mine])
    arrive(pl_copies)
    pl_all[mine, :] = plrx[0] + plrx[1] + plrx[2] + plrx[3] + att16 + bdown
    pl_copies = to_sp(pl_all.at[mine], pl_all.at[mine])
    hbg_copies = to_sp(hbg.at[:, mine], hbg.at[:, mine])
    bias_u = jnp.sum(u * bias_row, axis=1, keepdims=True)
    gain_u = u * gain_row
    uc_o[...] = (gain_u - row_mean(gain_u)).astype(BF16)
    arrive(go_copies)
    arrive(forward_copies)

    zmask = jnp.where(iota((SLOT, HDS), 0) == iota((SLOT, HDS), 1) // HD, 1.0, 0.0)
    for k in range(TP):
        def spread(b, k=k):
            zl[k, pl.ds(pl.multiple_of(b * SLOT, SLOT), SLOT), :] = go_all[k, pl.ds(b, 1), 0:HDS] * zmask
        pl.loop(0, IMGS, unroll=8)(spread)
        d_ref[k] = jnp.concatenate([go_all[k, :, TOK:], jnp.zeros((IMGS, TOK), F32)], axis=0).T[HD:HD + SLOT]
        wv_k = wv_all[k].astype(BF16)

        def z_step(i, k=k, wv_k=wv_k):
            rows = pl.ds(pl.multiple_of(i * 128, 128), 128)
            z_ref[k, rows, :] = nn(zl[k, rows, :].astype(BF16), wv_k)
        pl.loop(0, IMGS * SLOT // 128)(z_step)

    f_all = f_ref[...].reshape(SLOTS, TOK)
    d_all = d_ref[...].reshape(SLOTS, TOK)

    def back_step(b):
        lanes = pl.ds(pl.multiple_of(b * TOK, TOK), TOK)
        eight = pl.ds(pl.multiple_of(b * SLOT, SLOT), SLOT)
        z = jnp.concatenate([z_ref[k, eight, :] for k in range(TP)], axis=0)
        grad_p = fold(nt(hi_lo(z), hx[lanes]))
        bias_z = jnp.sum(z * bias_row, axis=1, keepdims=True)
        gain_z = z * gain_row
        z_o[b] = (gain_z - row_mean(gain_z)).astype(BF16)
        here = lane == b
        f_col = jnp.sum(jnp.where(here, f_all, 0.0), axis=1, keepdims=True)
        d_col = jnp.sum(jnp.where(here, d_all, 0.0), axis=1, keepdims=True)
        p = e_ref[:, :, lanes].reshape(SLOTS, TOK) * f_col
        ds = p * (grad_p - d_col) * SCALE
        raw = s_ref[:, :, lanes].reshape(SLOTS, TOK)
        terms = ds * (raw - bias_u) + p * (grad_p - bias_z)
        c2_o[pl.ds(b, 1), :] = jnp.sum(terms, axis=0, keepdims=True) * (1.0 / WIDTH)
        a_o[b] = jnp.concatenate([ds, p], axis=0).astype(BF16)
        e_ref[:, :, lanes] = ds.reshape(TP, SLOT, TOK)

    pl.loop(0, IMGS, unroll=2)(back_step)

    def r_step(i, acc):
        rows = pl.ds(pl.multiple_of(i * chunk, chunk), chunk)
        return acc + nn(hi_lo(e_ref[t, :, rows]), hx[rows])

    r_part = fold(lax.fori_loop(0, 8, r_step, jnp.zeros((2 * SLOT, WIDTH), F32)))
    rrx[s] = r_part
    r_copies = to_sp(rrx.at[s], rrx.at[s])

    def query_grad(r_rows):
        return jnp.sum(jnp.where(diag, fold(nt(hi_lo(r_rows), wk[...])), 0.0), axis=0, keepdims=True)

    gq_part = jnp.where(iota((SLOT, HDS), 0) == 0, query_grad(r_part), 0.0)
    gp_part = fold(nn(hi_lo(gq_part), wq[...]))
    slot = t * SP + s
    for i in range(WIDTH // TOK):
        gprx[slot, i:i + 1, :] = gp_part[0:1, i * TOK:(i + 1) * TOK]
    gp_copies = [remote(gprx.at[slot], gprx.at[slot], next(index), (dp, tps[k], sps[d])) for k in (2, 1, 3, 0) for d in (3, 2, 1, 0) if (k, d) != (0, 0)]

    arrive(pl_copies)
    pooled_o[...] = pl_all[...].astype(BF16)
    arrive(ga_copies)
    ga_o[...] = ga_all[...].astype(BF16)
    arrive(o_copies)
    o_o[...] = o_all[...].astype(BF16)
    go_o[...] = go_all[t].astype(BF16)
    arrive(hbg_copies)
    hb_o[...] = hbg[...].astype(BF16)
    arrive(r_copies)
    r_sum = rrx[0] + rrx[1] + rrx[2] + rrx[3]
    r_o[...] = r_sum
    gq_o[:, 0:HDS] = jnp.broadcast_to(query_grad(r_sum), (SLOT, HDS))
    arrive(gp_copies)
    gp_o[...] = sum(gprx[i] for i in range(TP * SP))
    for copy in started:
        copy.wait_send()


N_MESSAGES = 96


def middle(*args):
    vm, sds = pltpu.VMEM, jax.ShapeDtypeStruct
    outs = (sds((IMGS, WIDTH), BF16), sds((IMGS, 2 * SLOTS, TOK), BF16), sds((IMGS, SLOTS, WIDTH), BF16), sds((SLOTS, WIDTH), BF16), sds((IMGS, TOK), F32),
            sds((IMGS, WIDTH), BF16), sds((IMGS, WIDTH), BF16), sds((IMGS, WIDTH), BF16), sds((IMGS, WIDTH), BF16), sds((IMGS, 256), BF16), sds((IMGS, 256), BF16),
            sds((HEADS, IMGS, WIDTH), BF16), sds((SLOT, WIDTH), F32), sds((SLOT, 256), F32), sds((SLOT, 256), F32), sds((SLOT, TOK), F32))
    scratch = [vm((ROWS, WIDTH), BF16), vm((WIDTH, WIDTH), BF16), vm((WIDTH, WIDTH), BF16), vm((TP, SLOT, WIDTH), F32),
               vm((TP, SLOT, ROWS), F32), vm((TP, SLOT, ROWS), F32), vm((SP, 2 * SLOTS, TOK), F32), vm((TP, SLOT, TOK), F32), vm((TOK, SLOT), F32), vm((TP, SLOT, TOK), F32),
               vm((HEADS, IMGS, WIDTH), F32), vm((SP, HEADS, GROUP, WIDTH), F32), vm((HEADS, IMGS, WIDTH), F32),
               vm((TP, GROUP, WIDTH), F32), vm((IMGS, WIDTH), F32), vm((IMGS, 256), F32),
               vm((IMGS, WIDTH), F32), vm((TP, GROUP, WIDTH), F32), vm((IMGS, WIDTH), F32), vm((TP, GROUP, WIDTH), F32), vm((IMGS, WIDTH), F32),
               vm((TP, IMGS, 256), F32), vm((IMGS, WIDTH), F32), vm((TP, HDS, WIDTH), F32), vm((TP, IMGS * SLOT, HDS), F32), vm((TP, IMGS * SLOT, WIDTH), F32),
               vm((SP, SLOT, WIDTH), F32), vm((TP * SP, SLOT, TOK), F32),
               pltpu.SemaphoreType.DMA((10,)), pltpu.SemaphoreType.DMA((N_MESSAGES,)), pltpu.SemaphoreType.DMA((N_MESSAGES,))]
    any_spec, vm_spec = pl.BlockSpec(memory_space=pl.ANY), pl.BlockSpec(memory_space=vm)
    in_specs = [any_spec] + [vm_spec] * 14 + [any_spec] * 2 + [vm_spec]
    return pl.pallas_call(middle_kernel, out_shape=outs, in_specs=in_specs, out_specs=[vm_spec] * len(outs), scratch_shapes=scratch,
                          compiler_params=pltpu.CompilerParams(collective_id=0, has_side_effects=True, vmem_limit_bytes=60 * 1024 * 1024), name='middle')(*args)


STEPS = 8


def final_kernel(x_ref, a_ref, z_ref, uc_ref, c2_ref, y_ref, gpre_ref, hid_ref, og_ref, o_ref, ga_ref, go_ref, hb_ref, gq_ref, q_ref, r_ref, probe_ref, gp_ref, pool_ref,
                 gx_ref, gup_ref, gdown_ref, gout_ref, gvalue_ref, gquery_ref, gkey_ref, gprobe_ref, pooled_ref):
    step = pl.program_id(0)
    images = IMGS // STEPS
    c2_cols = jnp.concatenate([c2_ref[...]] * (TOK // images), axis=0).T
    for b in range(images):
        rows = slice(b * TOK, (b + 1) * TOK)
        mixed = tn(a_ref[b], jnp.concatenate([uc_ref[...], z_ref[b]], axis=0))
        x = x_ref[rows].astype(F32)
        centred = x - row_mean(x)
        inv = lax.rsqrt(row_mean(centred * centred) + NORM_EPS)
        gx_ref[rows] = (inv * mixed - centred * (inv * inv * c2_cols[:, b:b + 1])).astype(BF16)

    @pl.when(step < WIDTH // TOK)
    def _():
        gup_ref[...] = tn(y_ref[...], gpre_ref[...])
        gdown_ref[...] = tn(hid_ref[...], og_ref[...])

    @pl.when(step == 6)
    def _():
        gout_ref[...] = tn(o_ref[...], ga_ref[...])[:HDS]

    @pl.when(step == 5)
    def _():
        gquery_ref[...] = gq_ref[...].T[:HDS, 0:1] * probe_ref[...].reshape(1, WIDTH)
        query = q_ref[...].T
        for h in range(HEADS):
            gkey_ref[h * HD:(h + 1) * HD] = query[h * HD:(h + 1) * HD, 0:1] * r_ref[h:h + 1]
        for i in range(WIDTH // TOK):
            gprobe_ref[i * TOK:(i + 1) * TOK] = gp_ref[i]
        pooled_ref[...] = pool_ref[...]

    @pl.when(step == 7)
    def _():
        go = go_ref[...]
        for h in range(HEADS):
            gvalue_ref[h * HD:(h + 1) * HD] = tn(go, hb_ref[h])[h * HD:(h + 1) * HD]


def final(*args):
    sds = jax.ShapeDtypeStruct
    images = IMGS // STEPS
    last = WIDTH // TOK - 1

    def whole(shape):
        return pl.BlockSpec(shape, lambda i: (0,) * len(shape))

    cols = pl.BlockSpec((IMGS, TOK), lambda i: (0, jnp.minimum(i, last)))
    out_rows = pl.BlockSpec((TOK, WIDTH), lambda i: (jnp.minimum(i, last), 0))
    x_spec = pl.BlockSpec((images * TOK, WIDTH), lambda i: (i, 0))
    in_specs = [x_spec, pl.BlockSpec((images, 2 * SLOTS, TOK), lambda i: (i, 0, 0)), pl.BlockSpec((images, SLOTS, WIDTH), lambda i: (i, 0, 0)),
                whole((SLOTS, WIDTH)), pl.BlockSpec((images, TOK), lambda i: (i, 0)), cols, whole((IMGS, WIDTH)), cols, whole((IMGS, WIDTH)),
                whole((IMGS, 256)), whole((IMGS, WIDTH)), whole((IMGS, 256)), whole((HEADS, IMGS, WIDTH)),
                whole((SLOT, 256)), whole((SLOT, 256)), whole((SLOT, WIDTH)), whole((WIDTH,)), whole((SLOT, TOK)), whole((IMGS, WIDTH))]
    outs = (sds((ROWS, WIDTH), BF16), sds((WIDTH, WIDTH), F32), sds((WIDTH, WIDTH), F32), sds((HDS, WIDTH), F32), sds((HDS, WIDTH), F32), sds((HDS, WIDTH), F32), sds((HDS, WIDTH), F32), sds((WIDTH,), F32), sds((IMGS, WIDTH), BF16))
    out_specs = [x_spec, out_rows, out_rows] + [whole((HDS, WIDTH))] * 4 + [whole((WIDTH,)), whole((IMGS, WIDTH))]
    return pl.pallas_call(final_kernel, grid=(STEPS,), out_shape=outs, in_specs=in_specs, out_specs=out_specs,
                          compiler_params=pltpu.CompilerParams(dimension_semantics=('arbitrary',), vmem_limit_bytes=63 * 1024 * 1024), name='final')(*args)


def local_head(encoded, enc_gain, enc_bias, probe, w_query, b_query, w_key, w_value, b_value, w_out, b_out, head_gain, head_bias, w_up, b_up, w_down, b_down, out_grad):
    def flat(w):
        return jnp.transpose(w, (1, 2, 0)).reshape(HDS, WIDTH)

    def unflat(g):
        return jnp.transpose(g.reshape(HEADS, HD, WIDTH), (2, 0, 1))

    x = encoded.reshape(ROWS, WIDTH)
    pool, a, z, uc, c2, y, hid, gpre, ga, o, go, hb, r, gq, q, gp = middle(
        x, enc_gain, enc_bias, probe, flat(w_query), flat(w_key), flat(w_value), w_out.reshape(HDS, WIDTH), b_query, b_value,
        b_out, head_gain, head_bias, b_up, b_down, w_up, w_down, out_grad)
    grad_x, grad_w_up, grad_w_down, grad_w_out, grad_w_value, grad_w_query, grad_w_key, grad_probe, pooled = final(
        x, a, z, uc, c2, y, gpre, hid, out_grad, o, ga, go, hb, gq, q, r, probe, gp, pool)
    return (pooled, grad_x.reshape(IMGS, TOK, WIDTH), grad_probe, unflat(grad_w_query), unflat(grad_w_key), unflat(grad_w_value),
            grad_w_out.reshape(HEADS, HD, WIDTH), grad_w_up, grad_w_down)


def solution(mesh):
    return jax.shard_map(local_head, mesh=mesh, in_specs=IN_SPECS, out_specs=OUT_SPECS, check_vma=False)
```

```python
import functools
import jax
import jax.numpy as jnp
from jax import lax
from jax.experimental import pallas as pl
from jax.experimental.pallas import tpu as pltpu
from jax.sharding import PartitionSpec as P

NORM_EPS = 1e-6
IN_SPECS = (P('dp', 'sp', None), P(), P(), P(), P(None, 'tp', None), P('tp', None), P(None, 'tp', None), P(None, 'tp', None), P('tp', None), P('tp', None, None), P(), P(), P(), P(None, 'tp'), P('tp'), P('tp', None), P(), P('dp', None))
OUT_SPECS = (P('dp', None), P('dp', 'sp', None), P('dp'), P('dp', 'tp', None), P('dp', 'tp', None), P('dp', 'tp', None), P(('dp', 'tp'), None, None), P('dp', 'tp'), P(('dp', 'tp'), None))
F32, BF16 = jnp.float32, jnp.bfloat16
MESH = pl.DeviceIdType.MESH
IMGS, TOK, WIDTH, HD, HEADS, TP, SP = 64, 128, 768, 64, 3, 4, 4
ROWS = IMGS * TOK
HDS = HEADS * HD
GROUP = IMGS // SP
SLOT = 8
PAIRS = TP // 2
SLOTS = PAIRS * SLOT
QUARTER = HDS // 4
SCALE = HD ** -0.5


def dot(a, b, dims):
    return lax.dot_general(a, b, (dims, ((), ())), preferred_element_type=F32)


nn = functools.partial(dot, dims=((1,), (0,)))
nt = functools.partial(dot, dims=((1,), (1,)))
tn = functools.partial(dot, dims=((0,), (0,)))


def hi_lo(a):
    hi = a.astype(BF16).astype(F32)
    return jnp.concatenate([hi, a - hi], axis=0).astype(BF16)


def fold(a):
    half = a.shape[0] // 2
    return a[:half] + a[half:]


def row_mean(a):
    return jnp.mean(a, axis=-1, keepdims=True)


def iota(shape, axis):
    return lax.broadcasted_iota(jnp.int32, shape, axis)


def middle_kernel(x_hbm, gain_1d, bias_1d, probe_1d, wq, wk, wv, wo, bq_ref, bv_ref, bout_1d, hgain_1d, hbias_1d, bup_1d, bdown_1d, wup_hbm, wdown_hbm, og,
                  pooled_o, small_o, xh_o, a_o, z_o, uc_o, coef_o, y_o, hid_o, gpre_o, ga_o, o_o, go_o, hb_o,
                  hx, wup, wdown, u_rx, s_ref, e_ref, inv_ref, ml, f_ref, w_ref, d_ref, hb, hbrx, hbg, arx, att_all, o_all,
                  gnp, gnrx, plp, plrx, pl_all, ga_all, wv_all, go_all, zl, z_ref, a_s, z_s, uc_s, coef_s, y_s, hid_s, gpre_s, ga_s, hb_s, r_acc, rrx, gprx, lsem, ssem, rsem):
    dp, t, s = lax.axis_index('dp'), lax.axis_index('tp'), lax.axis_index('sp')
    s1 = s + 1 - 2 * lax.rem(s, 2)
    s2 = lax.rem(s + 2, 4)
    s3 = lax.rem(s1 + 2, 4)
    sps = (s, s1, s2, s3)
    tps = tuple(lax.rem(t + k, 4) for k in range(4))
    pair, odd = t // 2, lax.rem(t, 2)
    mine = pl.ds(pl.multiple_of(s * GROUP, GROUP), GROUP)
    started = []
    index = iter(range(N_MESSAGES))

    def remote(src, dst, device):
        sem = next(index)
        copy = pltpu.make_async_remote_copy(src_ref=src, dst_ref=dst, send_sem=ssem.at[sem], recv_sem=rsem.at[sem], device_id=device, device_id_type=MESH)
        copy.start()
        started.append(copy)
        return copy

    def to_tp(src, dst):
        return [remote(src, dst, (dp, tps[k], s)) for k in (2, 1, 3)]

    def to_sp(src, dst):
        return [remote(src, dst, (dp, t, sps[d])) for d in (3, 2, 1)]

    def arrive(copies):
        for copy in copies:
            copy.wait_recv()

    puts = []

    def put(src, dst):
        puts.append(pltpu.make_async_copy(src, dst, lsem.at[6 + len(puts)]))
        puts[-1].start()

    def own(rows):
        return jnp.where(odd == 1, pltpu.roll(rows, SLOT // 2, 0), rows)

    order = (3, 2, 1, 0)
    span = GROUP * TOK
    bases = [pl.multiple_of(sps[d] * span, span) for d in order]
    x_copies = [pltpu.make_async_copy(x_hbm.at[pl.ds(base, span)], hx.at[pl.ds(base, span)], lsem.at[i]) for i, base in enumerate(bases)]
    x_copies += [pltpu.make_async_copy(wup_hbm, wup, lsem.at[4]), pltpu.make_async_copy(wdown_hbm, wdown, lsem.at[5])]
    for copy in x_copies:
        copy.start()

    o_all[...] = jnp.zeros_like(o_all)
    go_all[...] = jnp.zeros_like(go_all)
    gprx[...] = jnp.zeros_like(gprx)
    barrier = pltpu.get_barrier_semaphore()
    peers = [(dp, tps[k], sps[d]) for k in range(4) for d in range(4) if (k, d) != (0, 0)]
    peers += [(1 - dp, t, s)]
    for peer in peers:
        pl.semaphore_signal(barrier, inc=1, device_id=peer, device_id_type=MESH)

    gain, bias, probe, bout, hgain, hbias, bup, bdown = [v[...].reshape(1, WIDTH) for v in (gain_1d, bias_1d, probe_1d, bout_1d, hgain_1d, hbias_1d, bup_1d, bdown_1d)]
    bq, bv = [jnp.concatenate([v[h:h + 1] for h in range(HEADS)], axis=1) for v in (bq_ref, bv_ref)]
    probe_rows = jnp.broadcast_to(probe, (16, WIDTH)).astype(BF16)
    query = (nt(probe_rows, wq[...]) + bq).astype(BF16).astype(F32)[:SLOT]
    slot_row, slot_lane = iota((SLOT, HDS), 0), iota((SLOT, HDS), 1) // HD

    def slots_of(parity):
        return (slot_row // 4 == parity) & (lax.rem(slot_row, 4) == slot_lane)

    diag = slots_of(0)
    u_rx[t] = fold(nn(hi_lo(jnp.where(slots_of(odd), query, 0.0)), wk[...]))
    wv_all[t] = wv[...].astype(F32)
    head_shift = fold(nt(hi_lo(jnp.broadcast_to(bias, (SLOT, WIDTH))), wv[...]))[0:1] + bv

    step_rows = 2 * TOK
    image_lane = iota((TOK, TOK), 1)

    def norm_step(i, base):
        rows = pl.ds(pl.multiple_of(base + i * step_rows, step_rows), step_rows)
        x = hx[rows].astype(F32)
        centred = x - row_mean(x)
        inv = lax.rsqrt(row_mean(centred * centred) + NORM_EPS)
        hx[rows] = (centred * inv).astype(BF16)
        image = base // TOK + 2 * i
        inv_ref[...] = jnp.where(image_lane == image, inv[:TOK], jnp.where(image_lane == image + 1, inv[TOK:], inv_ref[...]))

    def norm_group(i):
        x_copies[i].wait()
        pl.loop(0, span // step_rows)(functools.partial(norm_step, base=bases[i]))
        block = pl.ds(bases[i], span)
        put(hx.at[block], xh_o.at[block])

    norm_group(0)
    norm_group(1)
    pl.semaphore_wait(barrier, len(peers))
    u_copies = to_tp(u_rx.at[t], u_rx.at[t])
    quarters = [pl.ds(pl.multiple_of((lax.rem(s, 2) + 2 * x) * QUARTER, 16), QUARTER) for x in (dp, 1 - dp)]
    norm_group(2)
    norm_group(3)

    def relay_x(whole, copies):
        arrive(copies)
        blocks = [whole.at[tps[(4 - k) % 4], quarters[0]] for k in (2, 1, 3)]
        across = [remote(b, b, (1 - dp, t, s)) for b in blocks]
        return across, [remote(b, b, (dp, t, s1)) for b in blocks]

    def relay_core(whole, across):
        arrive(across)
        blocks = [whole.at[tps[(4 - k) % 4], quarters[1]] for k in (2, 1, 3)]
        return [remote(b, b, (dp, t, s1)) for b in blocks]

    arrive(u_copies)
    wv_copies = to_tp(wv_all.at[t, quarters[0]], wv_all.at[t, quarters[0]])
    u = jnp.concatenate([(u_rx[2 * k] + u_rx[2 * k + 1]) * gain for k in range(PAIRS)], axis=0)
    u_split = hi_lo(u)
    uc_s[...] = (u - row_mean(u)).astype(BF16)
    put(uc_s, uc_o)
    lane = iota((SLOTS, TOK), 1)
    wide = 4 * TOK

    def score_step(i, carry, base):
        m_all, l_all = carry
        start = pl.multiple_of(base + i * wide, wide)
        raw = fold(nt(u_split, hx[pl.ds(start, wide)]))
        s_ref[:, :, pl.ds(start, wide)] = raw.reshape(PAIRS, SLOT, wide)
        for j in range(wide // TOK):
            score = raw[:, j * TOK:(j + 1) * TOK] * SCALE
            top = jnp.max(score, axis=1, keepdims=True)
            e = jnp.exp(score - top)
            total = jnp.sum(e, axis=1, keepdims=True)
            e_ref[:, :, pl.ds(pl.multiple_of(start + j * TOK, TOK), TOK)] = e.reshape(PAIRS, SLOT, TOK)
            here = lane == i * (wide // TOK) + j
            m_all = jnp.where(here, top, m_all)
            l_all = jnp.where(here, total, l_all)
        return m_all, l_all

    def pooled_step(i, base):
        lanes = pl.ds(pl.multiple_of(base + i * TOK, TOK), TOK)
        result = fold(nn(hi_lo(own(e_ref[pair, :, lanes])), hx[lanes]))
        for h in range(HEADS):
            hb[h, pl.ds(base // TOK + i, 1), :] = result[h:h + 1]

    ml_copies, hb_copies = [], []
    for d, base in zip(order, bases):
        m_own, l_own = lax.fori_loop(0, span // wide, functools.partial(score_step, base=base), (jnp.zeros((SLOTS, TOK), F32), jnp.ones((SLOTS, TOK), F32)))
        ml[s, sps[d], 0:SLOTS] = m_own
        ml[s, sps[d], SLOTS:] = l_own
        ml_copies.append(to_sp(ml.at[s, sps[d]], ml.at[s, sps[d]]))
        pl.loop(0, GROUP, unroll=4)(functools.partial(pooled_step, base=base))
        group = pl.ds(pl.multiple_of(sps[d] * GROUP, GROUP), GROUP)
        if d:
            hb_copies.append(remote(hb.at[:, group], hbrx.at[s], (dp, t, sps[d])))
        else:
            hbrx[s] = hb[:, group, :]


    def weights_of(g, sources):
        tops = [ml[k, g, 0:SLOTS] for k in range(SP)]
        top = functools.reduce(jnp.maximum, tops)
        total = sum(ml[k, g, SLOTS:] * jnp.exp(tops[k] - top) for k in range(SP))
        return [jnp.exp(ml[k, g, 0:SLOTS] - top) / total for k in sources]

    for i, d in enumerate((3, 2, 1)):
        ml_copies[i][i].wait_recv()
    cols = []
    for k, weight in enumerate(weights_of(s, range(SP))):
        w_ref[k] = weight.reshape(PAIRS, SLOT, TOK)
        cols.append(own(w_ref[k, pair]).T)
    arrive(hb_copies)
    lane_head = iota((GROUP, HDS), 1) // HD
    o_part = jnp.zeros((GROUP, HDS), F32)
    for h in range(HEADS):
        hsum = sum(hbrx[k, h] * cols[k][0:GROUP, h:h + 1] for k in range(SP)) * gain
        hbg[h, mine, :] = hsum + bias
        o_part = jnp.where(lane_head == h, fold(nt(hi_lo(hsum), wv[...])), o_part)
    o_all[mine, 0:HDS] = o_part + head_shift
    arx[t] = nn((o_part + head_shift).astype(BF16), wo[...])
    att_copies = to_tp(arx.at[t], arx.at[t])
    wv_across, wv_core = relay_x(wv_all, wv_copies)
    x_copies[4].wait()
    x_copies[5].wait()
    grad_hidden = nt(og[...], wdown[...])
    for i, d in enumerate((3, 2, 1)):
        arrive([c for j, c in enumerate(ml_copies[i]) if j != i])
    arrive(ml_copies[3])
    for g in range(SP):
        f_ref[g] = weights_of(g, [s])[0]
    inv_ref[...] = inv_ref[...].T
    arrive(att_copies)
    att_all[mine, :] = arx[0] + arx[1] + arx[2] + arx[3] + bout
    att_copies = to_sp(att_all.at[mine], att_all.at[mine])
    o_copies = to_sp(o_all.at[mine], o_all.at[mine])
    arrive(att_copies)

    att = att_all[...]
    centred = att - row_mean(att)
    inv = lax.rsqrt(row_mean(centred * centred) + NORM_EPS)
    y = (centred * inv * hgain + hbias).astype(BF16)
    pre = nn(y, wup[...]) + bup
    square = pre * pre
    tanh = jnp.tanh((2 / jnp.pi) ** 0.5 * (pre + 0.044715 * (square * pre)))
    slope = 0.5 * (1.0 + tanh) + 0.5 * pre * (1.0 - tanh * tanh) * ((2 / jnp.pi) ** 0.5 * (1.0 + 3 * 0.044715 * square))
    gpre = (grad_hidden * slope).astype(BF16)
    gnp[...] = nt(gpre, wup[...])
    gnrx[t] = gnp[mine, :]
    gn_copies = to_tp(gnrx.at[t], gnrx.at[t])
    hid = (0.5 * pre * (1.0 + tanh)).astype(BF16)
    for value, kept, out in ((y, y_s, y_o), (gpre, gpre_s, gpre_o), (hid, hid_s, hid_o)):
        kept[...] = value
        put(kept, out)
    plp[...] = nn(hid, wdown[...])
    plrx[t] = plp[mine, :]
    wv_second = relay_core(wv_all, wv_across)
    arrive(gn_copies)
    grad_y = (gnrx[0] + gnrx[1] + gnrx[2] + gnrx[3]) * hgain
    att16 = att_all[mine, :]
    centred = att16 - row_mean(att16)
    inv = lax.rsqrt(row_mean(centred * centred) + NORM_EPS)
    unit = centred * inv
    grad_att = og[mine, :].astype(F32) + inv * (grad_y - row_mean(grad_y) - unit * row_mean(grad_y * unit))
    go = nt(grad_att.astype(BF16), wo[...]).astype(BF16).astype(F32)
    tail_lane = iota((GROUP, HD), 1)
    tail = jnp.zeros((GROUP, HD), F32)
    for h in range(HEADS):
        delta = jnp.sum(jnp.where(lane_head == h, go * o_part, 0.0), axis=1, keepdims=True)
        tail = jnp.where(tail_lane == h, delta, tail)
    go_all[t, mine, 0:HDS] = go
    go_all[t, mine, HDS:] = tail
    go_copies = to_tp(go_all.at[t, mine], go_all.at[t, mine])
    ga_all[mine, :] = grad_att
    arrive(go_copies)
    go_copies = to_sp(go_all.at[:, mine], go_all.at[:, mine])
    pl_copies = to_tp(plrx.at[t], plrx.at[t])
    arrive(wv_core)
    arrive(wv_second)
    arrive(go_copies)
    ga_copies = to_sp(ga_all.at[mine], ga_all.at[mine])
    hbg_copies = to_sp(hbg.at[:, mine], hbg.at[:, mine])

    for j in range(PAIRS):
        deltas = [jnp.concatenate([go_all[2 * j + k, :, TOK:], jnp.zeros((IMGS, TOK), F32)], axis=0).T[HD:HD + SLOT // 2] for k in range(2)]
        d_ref[j] = jnp.concatenate(deltas, axis=0)
    for k in range(TP):
        mask = jnp.where(slots_of(k % 2), 1.0, 0.0)

        def spread(b, k=k, mask=mask):
            zl[k, pl.ds(pl.multiple_of(b * SLOT, SLOT), SLOT), :] = go_all[k, pl.ds(b, 1), 0:HDS] * mask
        pl.loop(0, IMGS, unroll=8)(spread)
    for j in range(PAIRS):
        wv_pair = [wv_all[k].astype(BF16) for k in (2 * j, 2 * j + 1)]

        def z_step(i, j=j, wv_pair=wv_pair):
            rows = pl.ds(pl.multiple_of(i * 128, 128), 128)
            z_ref[j, rows, :] = sum(nn(zl[2 * j + k, rows, :].astype(BF16), wv_pair[k]) for k in range(2)) * gain
        pl.loop(0, IMGS * SLOT // 128)(z_step)

    d_all = d_ref[...].reshape(SLOTS, TOK)
    r_acc[...] = jnp.zeros_like(r_acc)

    batch = 4

    def back_step(i):
        images = [i * batch + j for j in range(batch)]
        rows = pl.ds(pl.multiple_of(i * batch * TOK, batch * TOK), batch * TOK)
        x = hx[rows]
        grads = []
        for j, b in enumerate(images):
            eight = pl.ds(pl.multiple_of(b * SLOT, SLOT), SLOT)
            z = jnp.concatenate([z_ref[k, eight, :] for k in range(PAIRS)], axis=0)
            grads.append(fold(nt(hi_lo(z), x[j * TOK:(j + 1) * TOK])))
            z_s[b] = (z - row_mean(z)).astype(BF16)
        all_ds = []
        for b, grad_p in zip(images, grads):
            lanes = pl.ds(pl.multiple_of(b * TOK, TOK), TOK)
            f_col = jnp.sum(jnp.where(lane == lax.rem(b, GROUP), f_ref[b // GROUP], 0.0), axis=1, keepdims=True)
            d_col = jnp.sum(jnp.where(lane == b, d_all, 0.0), axis=1, keepdims=True)
            p = e_ref[:, :, lanes].reshape(SLOTS, TOK) * f_col
            ds = p * (grad_p - d_col) * SCALE
            raw = s_ref[:, :, lanes].reshape(SLOTS, TOK)
            inv_row = inv_ref[pl.ds(b, 1), :]
            coef_s[pl.ds(b, 1), :] = jnp.sum(ds * raw + p * grad_p, axis=0, keepdims=True) * inv_row * (-1.0 / WIDTH)
            a_s[b] = (jnp.concatenate([ds, p], axis=0) * inv_row).astype(BF16)
            all_ds.append(own(jnp.where(pair == 1, ds[SLOT:], ds[:SLOT])))
        r_acc[...] += nn(hi_lo(jnp.concatenate(all_ds, axis=1)), x)

    for g in range(SP):
        pl.loop(g * GROUP // batch, (g + 1) * GROUP // batch)(back_step)
        group = pl.ds(g * GROUP, GROUP)
        put(a_s.at[group], a_o.at[group])
        put(z_s.at[group], z_o.at[group])
        if g == 0:
            arrive(pl_copies)
            pl_all[mine, :] = plrx[0] + plrx[1] + plrx[2] + plrx[3] + att_all[mine, :] + bdown
            pl_copies = to_sp(pl_all.at[mine], pl_all.at[mine])
            put(go_all.at[t], go_o)
        if g == 2:
            arrive(o_copies)
            put(o_all, o_o)
            arrive(ga_copies)
            ga_s[...] = ga_all[...].astype(BF16)
            put(ga_s, ga_o)
    put(coef_s, coef_o)

    r_part = fold(r_acc[...]) * gain
    rrx[s] = r_part
    r_copies = to_sp(rrx.at[s], rrx.at[s])

    def query_grad(r_rows):
        return jnp.sum(jnp.where(diag, fold(nt(hi_lo(r_rows), wk[...])), 0.0), axis=0, keepdims=True)

    gq_part = jnp.where(iota((SLOT, HDS), 0) == 0, query_grad(r_part), 0.0)
    gp_part = fold(nn(hi_lo(gq_part), wq[...]))
    slot = t * SP + s
    for i in range(WIDTH // TOK):
        gprx[slot, i:i + 1, :] = gp_part[0:1, i * TOK:(i + 1) * TOK]
    gp_copies = [remote(gprx.at[slot], gprx.at[slot], (dp, tps[k], sps[d])) for k in (2, 1, 3, 0) for d in (3, 2, 1, 0) if (k, d) != (0, 0)]

    arrive(pl_copies)
    pooled_o[...] = pl_all[...].astype(BF16)
    arrive(hbg_copies)
    hb_s[...] = hbg[...].astype(BF16)
    put(hb_s, hb_o)
    arrive(r_copies)
    r_sum = rrx[0] + rrx[1] + rrx[2] + rrx[3]
    small_o[...] = r_sum
    small_o[3:4, :] = jnp.zeros((1, WIDTH), F32)
    small_o[4:5, :] = jnp.zeros((1, WIDTH), F32)
    small_o[3:4, 0:HDS] = query_grad(r_sum)
    small_o[4:5, 0:HDS] = query[0:1]
    arrive(gp_copies)
    gp = sum(gprx[i] for i in range(TP * SP))
    for i in range(WIDTH // TOK):
        small_o[5:6, i * TOK:(i + 1) * TOK] = gp[i:i + 1]
    for copy in started:
        copy.wait_send()
    for copy in puts:
        copy.wait()


N_MESSAGES = 112


def middle(*args):
    vm, sds = pltpu.VMEM, jax.ShapeDtypeStruct
    wide = sds((IMGS, WIDTH), BF16)
    outs = (wide, sds((SLOT, WIDTH), F32), sds((ROWS, WIDTH), BF16), sds((IMGS, 2 * SLOTS, TOK), BF16), sds((IMGS, SLOTS, WIDTH), BF16), sds((SLOTS, WIDTH), BF16), sds((IMGS, TOK), F32),
            wide, wide, wide, wide, sds((IMGS, 256), F32), sds((IMGS, 256), F32), sds((HEADS, IMGS, WIDTH), BF16))
    scratch = [vm((ROWS, WIDTH), BF16), vm((WIDTH, WIDTH), BF16), vm((WIDTH, WIDTH), BF16), vm((TP, SLOT, WIDTH), F32),
               vm((PAIRS, SLOT, ROWS), F32), vm((PAIRS, SLOT, ROWS), F32), vm((TOK, TOK), F32), vm((SP, SP, 2 * SLOTS, TOK), F32), vm((SP, SLOTS, TOK), F32), vm((SP, PAIRS, SLOT, TOK), F32), vm((PAIRS, SLOT, TOK), F32),
               vm((HEADS, IMGS, WIDTH), F32), vm((SP, HEADS, GROUP, WIDTH), F32), vm((HEADS, IMGS, WIDTH), F32),
               vm((TP, GROUP, WIDTH), F32), vm((IMGS, WIDTH), F32), vm((IMGS, 256), F32),
               vm((IMGS, WIDTH), F32), vm((TP, GROUP, WIDTH), F32), vm((IMGS, WIDTH), F32), vm((TP, GROUP, WIDTH), F32), vm((IMGS, WIDTH), F32),
               vm((IMGS, WIDTH), F32), vm((TP, HDS, WIDTH), F32), vm((TP, IMGS, 256), F32), vm((TP, IMGS * SLOT, HDS), F32), vm((PAIRS, IMGS * SLOT, WIDTH), F32),
               vm((IMGS, 2 * SLOTS, TOK), BF16), vm((IMGS, SLOTS, WIDTH), BF16), vm((SLOTS, WIDTH), BF16), vm((IMGS, TOK), F32),
               vm((IMGS, WIDTH), BF16), vm((IMGS, WIDTH), BF16), vm((IMGS, WIDTH), BF16), vm((IMGS, WIDTH), BF16), vm((HEADS, IMGS, WIDTH), BF16), vm((2 * SLOT, WIDTH), F32),
               vm((SP, SLOT, WIDTH), F32), vm((TP * SP, SLOT, TOK), F32),
               pltpu.SemaphoreType.DMA((32,)), pltpu.SemaphoreType.DMA((N_MESSAGES,)), pltpu.SemaphoreType.DMA((N_MESSAGES,))]
    any_spec, vm_spec = pl.BlockSpec(memory_space=pl.ANY), pl.BlockSpec(memory_space=vm)
    in_specs = [any_spec] + [vm_spec] * 14 + [any_spec] * 2 + [vm_spec]
    out_specs = [vm_spec] * 2 + [any_spec] * (len(outs) - 2)
    return pl.pallas_call(middle_kernel, out_shape=outs, in_specs=in_specs, out_specs=out_specs, scratch_shapes=scratch,
                          compiler_params=pltpu.CompilerParams(collective_id=0, has_side_effects=True, vmem_limit_bytes=63 * 1024 * 1024), name='middle')(*args)


STEPS = 8


def final_kernel(xh_ref, a_ref, z_ref, uc_ref, coef_ref, y_ref, gpre_ref, hid_ref, og_ref, o_ref, ga_ref, go_ref, hb_ref, small_ref, probe_ref, pool_ref,
                 gx_ref, gup_ref, gdown_ref, gout_ref, gvalue_ref, gquery_ref, gkey_ref, gprobe_ref, pooled_ref):
    step = pl.program_id(0)
    images = IMGS // STEPS
    cols = jnp.concatenate([coef_ref[...]] * (TOK // images), axis=0).T
    for b in range(images):
        rows = slice(b * TOK, (b + 1) * TOK)
        mixed = tn(a_ref[b], jnp.concatenate([uc_ref[...], z_ref[b]], axis=0))
        gx_ref[rows] = (mixed + xh_ref[rows].astype(F32) * cols[:, b:b + 1]).astype(BF16)

    @pl.when(step < WIDTH // TOK)
    def _():
        gup_ref[...] = tn(y_ref[...], gpre_ref[...])
        gdown_ref[...] = tn(hid_ref[...], og_ref[...])

    @pl.when(step == 6)
    def _():
        gout_ref[...] = tn(o_ref[...].astype(BF16), ga_ref[...])[:HDS]

    @pl.when(step == 5)
    def _():
        turned = jnp.concatenate([small_ref[...], jnp.zeros((TOK - SLOT, WIDTH), F32)], axis=0)[:, :256].T
        gquery_ref[...] = turned[:HDS, 3:4] * probe_ref[...].reshape(1, WIDTH)
        for h in range(HEADS):
            gkey_ref[h * HD:(h + 1) * HD] = turned[h * HD:(h + 1) * HD, 4:5] * small_ref[h:h + 1]
        gprobe_ref[...] = small_ref[5]
        pooled_ref[...] = pool_ref[...]

    @pl.when(step == 7)
    def _():
        go = go_ref[...].astype(BF16)
        for h in range(HEADS):
            gvalue_ref[h * HD:(h + 1) * HD] = tn(go, hb_ref[h])[h * HD:(h + 1) * HD]


def final(*args):
    sds = jax.ShapeDtypeStruct
    images = IMGS // STEPS
    last = WIDTH // TOK - 1

    def whole(shape):
        return pl.BlockSpec(shape, lambda i: (0,) * len(shape))

    cols = pl.BlockSpec((IMGS, TOK), lambda i: (0, jnp.minimum(i, last)))
    out_rows = pl.BlockSpec((TOK, WIDTH), lambda i: (jnp.minimum(i, last), 0))
    x_spec = pl.BlockSpec((images * TOK, WIDTH), lambda i: (i, 0))
    in_specs = [x_spec, pl.BlockSpec((images, 2 * SLOTS, TOK), lambda i: (i, 0, 0)), pl.BlockSpec((images, SLOTS, WIDTH), lambda i: (i, 0, 0)),
                whole((SLOTS, WIDTH)), pl.BlockSpec((images, TOK), lambda i: (i, 0)), cols, whole((IMGS, WIDTH)), cols, whole((IMGS, WIDTH)),
                whole((IMGS, 256)), whole((IMGS, WIDTH)), whole((IMGS, 256)), whole((HEADS, IMGS, WIDTH)),
                whole((SLOT, WIDTH)), whole((WIDTH,)), whole((IMGS, WIDTH))]
    outs = (sds((ROWS, WIDTH), BF16), sds((WIDTH, WIDTH), F32), sds((WIDTH, WIDTH), F32), sds((HDS, WIDTH), F32), sds((HDS, WIDTH), F32), sds((HDS, WIDTH), F32), sds((HDS, WIDTH), F32), sds((WIDTH,), F32), sds((IMGS, WIDTH), BF16))
    out_specs = [x_spec, out_rows, out_rows] + [whole((HDS, WIDTH))] * 4 + [whole((WIDTH,)), whole((IMGS, WIDTH))]
    return pl.pallas_call(final_kernel, grid=(STEPS,), out_shape=outs, in_specs=in_specs, out_specs=out_specs,
                          compiler_params=pltpu.CompilerParams(dimension_semantics=('arbitrary',), vmem_limit_bytes=63 * 1024 * 1024), name='final')(*args)


def local_head(encoded, enc_gain, enc_bias, probe, w_query, b_query, w_key, w_value, b_value, w_out, b_out, head_gain, head_bias, w_up, b_up, w_down, b_down, out_grad):
    def flat(w):
        return jnp.transpose(w, (1, 2, 0)).reshape(HDS, WIDTH)

    def unflat(g):
        return jnp.transpose(g.reshape(HEADS, HD, WIDTH), (2, 0, 1))

    x = encoded.reshape(ROWS, WIDTH)
    pool, small, xh, a, z, uc, coef, y, hid, gpre, ga, o, go, hb = middle(
        x, enc_gain, enc_bias, probe, flat(w_query), flat(w_key), flat(w_value), w_out.reshape(HDS, WIDTH), b_query, b_value,
        b_out, head_gain, head_bias, b_up, b_down, w_up, w_down, out_grad)
    grad_x, grad_w_up, grad_w_down, grad_w_out, grad_w_value, grad_w_query, grad_w_key, grad_probe, pooled = final(
        xh, a, z, uc, coef, y, gpre, hid, out_grad, o, ga, go, hb, small, probe, pool)
    return (pooled, grad_x.reshape(IMGS, TOK, WIDTH), grad_probe, unflat(grad_w_query), unflat(grad_w_key), unflat(grad_w_value),
            grad_w_out.reshape(HEADS, HD, WIDTH), grad_w_up, grad_w_down)


def solution(mesh):
    return jax.shard_map(local_head, mesh=mesh, in_specs=IN_SPECS, out_specs=OUT_SPECS, check_vma=False)
```

```python
import functools
import jax
import jax.numpy as jnp
from jax import lax
from jax.experimental import pallas as pl
from jax.experimental.pallas import tpu as pltpu
from jax.sharding import PartitionSpec as P

NORM_EPS = 1e-6
IN_SPECS = (P('dp', 'sp', None), P(), P(), P(), P(None, 'tp', None), P('tp', None), P(None, 'tp', None), P(None, 'tp', None), P('tp', None), P('tp', None, None), P(), P(), P(), P(None, 'tp'), P('tp'), P('tp', None), P(), P('dp', None))
OUT_SPECS = (P('dp', None), P('dp', 'sp', None), P('dp'), P('dp', 'tp', None), P('dp', 'tp', None), P('dp', 'tp', None), P(('dp', 'tp'), None, None), P('dp', 'tp'), P(('dp', 'tp'), None))
F32, BF16 = jnp.float32, jnp.bfloat16
MESH = pl.DeviceIdType.MESH
IMGS, TOK, WIDTH, HD, HEADS, TP, SP = 64, 128, 768, 64, 3, 4, 4
ROWS = IMGS * TOK
HDS = HEADS * HD
GROUP = IMGS // SP
SLOT = 8
PAIRS = TP // 2
SLOTS = PAIRS * SLOT
QUARTER = HDS // 4
SCALE = HD ** -0.5


def dot(a, b, dims):
    return lax.dot_general(a, b, (dims, ((), ())), preferred_element_type=F32)


nn = functools.partial(dot, dims=((1,), (0,)))
nt = functools.partial(dot, dims=((1,), (1,)))
tn = functools.partial(dot, dims=((0,), (0,)))


def hi_lo(a):
    hi = a.astype(BF16).astype(F32)
    return jnp.concatenate([hi, a - hi], axis=0).astype(BF16)


def fold(a):
    half = a.shape[0] // 2
    return a[:half] + a[half:]


def row_mean(a):
    return jnp.mean(a, axis=-1, keepdims=True)


def iota(shape, axis):
    return lax.broadcasted_iota(jnp.int32, shape, axis)


def middle_kernel(x_hbm, gain_1d, bias_1d, probe_1d, wq, wk, wv, wo, bq_ref, bv_ref, bout_1d, hgain_1d, hbias_1d, bup_1d, bdown_1d, wup_hbm, wdown_hbm, og,
                  pooled_o, small_o, xh_o, a_o, z_o, uc_o, coef_o, y_o, hid_o, gpre_o, ga_o, o_o, go_o, hb_o,
                  xin, h0, h1, h2, h3, wup, wdown, u_rx, sg0, sg1, sg2, sg3, eg0, eg1, eg2, eg3, inv_ref, ml, f_ref, w_ref, d_ref, hb, hbrx, hbg, arx, att_all, o_all,
                  gh_ref, gnrx, plrx, pl_all, ga_all, wv_all, go_all, zl, z_ref, a_s, z_s, uc_s, coef_s, y_s, hid_s, gpre_s, ga_s, hb_s, pool_s, small_s, r_acc, rrx, gprx, lsem, ssem, rsem):
    dp, t, s = lax.axis_index('dp'), lax.axis_index('tp'), lax.axis_index('sp')
    s1 = s + 1 - 2 * lax.rem(s, 2)
    s2 = lax.rem(s + 2, 4)
    s3 = lax.rem(s1 + 2, 4)
    sps = (s, s1, s2, s3)
    tps = tuple(lax.rem(t + k, 4) for k in range(4))
    pair, odd = t // 2, lax.rem(t, 2)
    mine = pl.ds(pl.multiple_of(s * GROUP, GROUP), GROUP)
    started = []
    index = iter(range(N_MESSAGES))

    def remote(src, dst, device):
        sem = next(index)
        copy = pltpu.make_async_remote_copy(src_ref=src, dst_ref=dst, send_sem=ssem.at[sem], recv_sem=rsem.at[sem], device_id=device, device_id_type=MESH)
        copy.start()
        started.append(copy)
        return copy

    def to_tp(src, dst):
        return [remote(src, dst, (dp, tps[k], s)) for k in (2, 1, 3)]

    def to_sp(src, dst):
        return [remote(src, dst, (dp, t, sps[d])) for d in (3, 2, 1)]

    def arrive(copies):
        for copy in copies:
            copy.wait_recv()

    puts = []

    def put(src, dst):
        puts.append(pltpu.make_async_copy(src, dst, lsem.at[6 + len(puts)]))
        puts[-1].start()

    def own(rows):
        return jnp.where(odd == 1, pltpu.roll(rows, SLOT // 2, 0), rows)

    order = (3, 2, 1, 0)
    span = GROUP * TOK
    bases = [pl.multiple_of(sps[d] * span, span) for d in order]
    x_copies = [pltpu.make_async_copy(x_hbm.at[pl.ds(base, span)], xin.at[pl.ds(i * span, span)], lsem.at[i]) for i, base in enumerate(bases)]
    normed, raws, exps = (h0, h1, h2, h3), (sg0, sg1, sg2, sg3), (eg0, eg1, eg2, eg3)
    x_copies += [pltpu.make_async_copy(wup_hbm, wup, lsem.at[4]), pltpu.make_async_copy(wdown_hbm, wdown, lsem.at[5])]
    for copy in x_copies:
        copy.start()

    o_all[...] = jnp.zeros_like(o_all)
    go_all[...] = jnp.zeros_like(go_all)
    gprx[...] = jnp.zeros_like(gprx)
    barrier = pltpu.get_barrier_semaphore()
    peers = [(dp, tps[k], sps[d]) for k in range(4) for d in range(4) if (k, d) != (0, 0)]
    peers += [(1 - dp, t, s)]
    for peer in peers:
        pl.semaphore_signal(barrier, inc=1, device_id=peer, device_id_type=MESH)

    gain, bias, probe, bout, hgain, hbias, bup, bdown = [v[...].reshape(1, WIDTH) for v in (gain_1d, bias_1d, probe_1d, bout_1d, hgain_1d, hbias_1d, bup_1d, bdown_1d)]
    bq, bv = [jnp.concatenate([v[h:h + 1] for h in range(HEADS)], axis=1) for v in (bq_ref, bv_ref)]
    probe_rows = jnp.broadcast_to(probe, (16, WIDTH)).astype(BF16)
    query = (nt(probe_rows, wq[...]) + bq).astype(BF16).astype(F32)[:SLOT]
    slot_row, slot_lane = iota((SLOT, HDS), 0), iota((SLOT, HDS), 1) // HD

    def slots_of(parity):
        return (slot_row // 4 == parity) & (lax.rem(slot_row, 4) == slot_lane)

    diag = slots_of(0)
    u_rx[t] = fold(nn(hi_lo(jnp.where(slots_of(odd), query, 0.0)), wk[...]))
    wv_all[t] = wv[...].astype(F32)
    head_shift = fold(nt(hi_lo(jnp.broadcast_to(bias, (SLOT, WIDTH))), wv[...]))[0:1] + bv

    norm_rows = 2 * TOK
    image_lane = iota((TOK, TOK), 1)

    def norm_step(i, n):
        rows = slice(i * norm_rows, (i + 1) * norm_rows)
        x = xin[n * span + i * norm_rows:n * span + (i + 1) * norm_rows].astype(F32)
        centred = x - row_mean(x)
        inv = lax.rsqrt(row_mean(centred * centred) + NORM_EPS)
        normed[n][rows] = (centred * inv).astype(BF16)
        image = n * GROUP + 2 * i
        inv_ref[...] = jnp.where(image_lane == image, inv[:TOK], jnp.where(image_lane == image + 1, inv[TOK:], inv_ref[...]))

    def norm_steps(i, n):
        norm_step(2 * i, n)
        norm_step(2 * i + 1, n)

    def norm_done(n):
        put(normed[n], xh_o.at[pl.ds(bases[n], span)])

    pl.semaphore_wait(barrier, len(peers))
    u_copies = to_tp(u_rx.at[t], u_rx.at[t])
    x_copies[0].wait()
    for i in range(span // norm_rows // 2):
        norm_steps(i, 0)
    norm_done(0)
    quarters = [pl.ds(pl.multiple_of((lax.rem(s, 2) + 2 * x) * QUARTER, 16), QUARTER) for x in (dp, 1 - dp)]

    def relay_x(whole, copies):
        arrive(copies)
        blocks = [whole.at[tps[(4 - k) % 4], quarters[0]] for k in (2, 1, 3)]
        across = [remote(b, b, (1 - dp, t, s)) for b in blocks]
        return across, [remote(b, b, (dp, t, s1)) for b in blocks]

    def relay_core(whole, across):
        arrive(across)
        blocks = [whole.at[tps[(4 - k) % 4], quarters[1]] for k in (2, 1, 3)]
        return [remote(b, b, (dp, t, s1)) for b in blocks]

    arrive(u_copies)
    wv_copies = to_tp(wv_all.at[t, quarters[0]], wv_all.at[t, quarters[0]])
    u = jnp.concatenate([(u_rx[2 * k] + u_rx[2 * k + 1]) * gain for k in range(PAIRS)], axis=0)
    u_split = hi_lo(u)
    uc_s[...] = (u - row_mean(u)).astype(BF16)
    put(uc_s, uc_o)
    lane = iota((SLOTS, TOK), 1)
    wide = 4 * TOK

    def score_step(i, carry, n):
        m_all, l_all = carry
        raw = fold(nt(u_split, normed[n][i * wide:(i + 1) * wide]))
        raws[n][:, :, i * wide:(i + 1) * wide] = raw.reshape(PAIRS, SLOT, wide)
        for j in range(wide // TOK):
            score = raw[:, j * TOK:(j + 1) * TOK] * SCALE
            top = jnp.max(score, axis=1, keepdims=True)
            e = jnp.exp(score - top)
            total = jnp.sum(e, axis=1, keepdims=True)
            exps[n][:, :, i * wide + j * TOK:i * wide + (j + 1) * TOK] = e.reshape(PAIRS, SLOT, TOK)
            here = lane == i * (wide // TOK) + j
            m_all = jnp.where(here, top, m_all)
            l_all = jnp.where(here, total, l_all)
        return m_all, l_all

    def scores(n, ahead):
        carry = (jnp.zeros((SLOTS, TOK), F32), jnp.ones((SLOTS, TOK), F32))
        for i in range(span // wide):
            carry = score_step(i, carry, n)
            if ahead is not None:
                norm_steps(i, ahead)
        return carry

    def sums(n, ahead):
        for i in range(GROUP):
            lanes = slice(i * TOK, (i + 1) * TOK)
            result = fold(nn(hi_lo(own(exps[n][pair, :, lanes])), normed[n][lanes]))
            for h in range(HEADS):
                hb[n, h, i:i + 1, :] = result[h:h + 1]
            if ahead is not None and i % 4 == 3:
                norm_steps(i // 4, ahead)

    ml_copies, hb_copies = [], []
    for n, (d, base) in enumerate(zip(order, bases)):
        ahead = {0: (1, 2), 1: (3, None)}.get(n, (None, None))
        for a in ahead:
            if a is not None:
                x_copies[a].wait()
        m_own, l_own = scores(n, ahead[0])
        ml[s, sps[d], 0:SLOTS] = m_own
        ml[s, sps[d], SLOTS:] = l_own
        ml_copies.append(to_sp(ml.at[s, sps[d]], ml.at[s, sps[d]]))
        sums(n, ahead[1])
        for a in ahead:
            if a is not None:
                norm_done(a)
        if d:
            hb_copies.append(remote(hb.at[n], hbrx.at[s], (dp, t, sps[d])))
        else:
            hbrx[s] = hb[n]

    def weights_of(g, sources):
        tops = [ml[k, g, 0:SLOTS] for k in range(SP)]
        top = functools.reduce(jnp.maximum, tops)
        total = sum(ml[k, g, SLOTS:] * jnp.exp(tops[k] - top) for k in range(SP))
        return [jnp.exp(ml[k, g, 0:SLOTS] - top) / total for k in sources]

    for i, d in enumerate((3, 2, 1)):
        ml_copies[i][i].wait_recv()
    cols = []
    for k, weight in enumerate(weights_of(s, range(SP))):
        w_ref[k] = weight.reshape(PAIRS, SLOT, TOK)
        cols.append(own(w_ref[k, pair]).T)
    arrive(hb_copies)
    lane_head = iota((GROUP, HDS), 1) // HD
    o_part = jnp.zeros((GROUP, HDS), F32)
    for h in range(HEADS):
        hsum = sum(hbrx[k, h] * cols[k][0:GROUP, h:h + 1] for k in range(SP)) * gain
        hbg[h, mine, :] = hsum + bias
        o_part = jnp.where(lane_head == h, fold(nt(hi_lo(hsum), wv[...])), o_part)
    o_all[mine, 0:HDS] = o_part + head_shift
    arx[t] = nn((o_part + head_shift).astype(BF16), wo[...])
    att_copies = to_tp(arx.at[t], arx.at[t])
    hbg_copies = to_sp(hbg.at[:, mine], hbg.at[:, mine])
    wv_across, wv_core = relay_x(wv_all, wv_copies)
    x_copies[4].wait()
    x_copies[5].wait()
    grad_hidden = nt(og[...], wdown[...])
    gh_ref[...] = grad_hidden
    for i, d in enumerate((3, 2, 1)):
        arrive([c for j, c in enumerate(ml_copies[i]) if j != i])
    arrive(ml_copies[3])
    for g in range(SP):
        f_ref[g] = weights_of(sps[3 - g], [s])[0]
    inv_ref[...] = inv_ref[...].T
    arrive(att_copies)
    att16 = arx[0] + arx[1] + arx[2] + arx[3] + bout
    att_all[mine, :] = att16

    def mlp(att, grad_hidden):
        centred = att - row_mean(att)
        inv = lax.rsqrt(row_mean(centred * centred) + NORM_EPS)
        unit = centred * inv
        y = (unit * hgain + hbias).astype(BF16)
        pre = nn(y, wup[...]) + bup
        square = pre * pre
        tanh = jnp.tanh((2 / jnp.pi) ** 0.5 * (pre + 0.044715 * (square * pre)))
        slope = 0.5 * (1.0 + tanh) + 0.5 * pre * (1.0 - tanh * tanh) * ((2 / jnp.pi) ** 0.5 * (1.0 + 3 * 0.044715 * square))
        gpre = (grad_hidden * slope).astype(BF16)
        hid = (0.5 * pre * (1.0 + tanh)).astype(BF16)
        return inv, unit, y, gpre, hid

    inv, unit, _, gpre, hid = mlp(att16, gh_ref[mine, :])
    gnrx[t] = nt(gpre, wup[...])
    gn_copies = to_tp(gnrx.at[t], gnrx.at[t])
    att_copies = to_sp(att_all.at[mine], att_all.at[mine])
    o_copies = to_sp(o_all.at[mine], o_all.at[mine])
    plrx[t] = nn(hid, wdown[...])
    arrive(gn_copies)
    grad_y = (gnrx[0] + gnrx[1] + gnrx[2] + gnrx[3]) * hgain
    grad_att = og[mine, :].astype(F32) + inv * (grad_y - row_mean(grad_y) - unit * row_mean(grad_y * unit))
    go = nt(grad_att.astype(BF16), wo[...]).astype(BF16).astype(F32)
    tail_lane = iota((GROUP, HD), 1)
    tail = jnp.zeros((GROUP, HD), F32)
    for h in range(HEADS):
        delta = jnp.sum(jnp.where(lane_head == h, go * o_part, 0.0), axis=1, keepdims=True)
        tail = jnp.where(tail_lane == h, delta, tail)
    go_all[t, mine, 0:HDS] = go
    go_all[t, mine, HDS:] = tail
    go_copies = to_tp(go_all.at[t, mine], go_all.at[t, mine])
    ga_all[mine, :] = grad_att
    ga_copies = to_sp(ga_all.at[mine], ga_all.at[mine])
    wv_second = relay_core(wv_all, wv_across)
    arrive(att_copies)
    _, _, y, gpre, hid = mlp(att_all[...], gh_ref[...])
    for value, kept, out in ((y, y_s, y_o), (gpre, gpre_s, gpre_o), (hid, hid_s, hid_o)):
        kept[...] = value
        put(kept, out)
    arrive(wv_core)
    arrive(wv_second)
    arrive(go_copies)
    go_copies = to_sp(go_all.at[:, mine], go_all.at[:, mine])
    pl_copies = to_tp(plrx.at[t], plrx.at[t])

    def z_group(g, n):
        block = [go_all[k, pl.ds(pl.multiple_of(g * GROUP, GROUP), GROUP)] for k in range(TP)]
        for j in range(PAIRS):
            deltas = [jnp.concatenate([block[2 * j + k][:, TOK:], jnp.zeros((TOK - GROUP, TOK), F32)], axis=0).T[HD:HD + SLOT // 2] for k in range(2)]
            d_ref[n, j] = jnp.concatenate(deltas, axis=0)
        for k in range(TP):
            mask = jnp.where(slots_of(k % 2), 1.0, 0.0)
            for i in range(GROUP):
                zl[n, k, i * SLOT:(i + 1) * SLOT, :] = block[k][i:i + 1, 0:HDS] * mask
        for j in range(PAIRS):
            z_ref[n, j] = sum(nn(zl[n, 2 * j + k].astype(BF16), wv_all[2 * j + k].astype(BF16)) for k in range(2)) * gain

    r_acc[...] = jnp.zeros_like(r_acc)
    batch = 4

    def back_step(i, g, n):
        x = normed[n][i * batch * TOK:(i + 1) * batch * TOK]
        grads = []
        for j in range(batch):
            image = i * batch + j
            z = jnp.concatenate([z_ref[n, k, image * SLOT:(image + 1) * SLOT] for k in range(PAIRS)], axis=0)
            grads.append(fold(nt(hi_lo(z), x[j * TOK:(j + 1) * TOK])))
            z_s[n * GROUP + image] = (z - row_mean(z)).astype(BF16)
        all_ds = []
        for j, grad_p in enumerate(grads):
            image = i * batch + j
            lanes = slice(image * TOK, (image + 1) * TOK)
            f_col = f_ref[n][:, image:image + 1]
            d_col = d_ref[n].reshape(SLOTS, TOK)[:, image:image + 1]
            p = exps[n][:, :, lanes].reshape(SLOTS, TOK) * f_col
            ds = p * (grad_p - d_col) * SCALE
            raw = raws[n][:, :, lanes].reshape(SLOTS, TOK)
            row = n * GROUP + image
            inv_row = inv_ref[row:row + 1, :]
            coef_s[row:row + 1, :] = jnp.sum(ds * raw + p * grad_p, axis=0, keepdims=True) * inv_row * (-1.0 / WIDTH)
            a_s[row] = (jnp.concatenate([ds, p], axis=0) * inv_row).astype(BF16)
            all_ds.append(own(jnp.where(pair == 1, ds[SLOT:], ds[:SLOT])))
        return nn(hi_lo(jnp.concatenate(all_ds, axis=1)), x)

    steps = (0, 1, 3, 2)
    z_group(sps[0], 3)
    for turn, d in enumerate(steps):
        g, n = sps[d], 3 - d
        r_acc[...] += sum(back_step(i, g, n) for i in range(GROUP // batch))
        if d == 0:
            arrive(go_copies)
            arrive(pl_copies)
            pl_all[mine, :] = plrx[0] + plrx[1] + plrx[2] + plrx[3] + att16 + bdown
            pl_copies = to_sp(pl_all.at[mine], pl_all.at[mine])
        if turn < 3:
            z_group(sps[steps[turn + 1]], 3 - steps[turn + 1])
        group, kept = pl.ds(pl.multiple_of(g * GROUP, GROUP), GROUP), pl.ds(n * GROUP, GROUP)
        put(a_s.at[kept], a_o.at[group])
        put(z_s.at[kept], z_o.at[group])
        put(coef_s.at[kept], coef_o.at[group])
    arrive(o_copies)
    put(o_all, o_o)
    put(go_all.at[t], go_o)

    r_part = fold(r_acc[...]) * gain
    rrx[s] = r_part
    r_copies = to_sp(rrx.at[s], rrx.at[s])

    def query_grad(r_rows):
        return jnp.sum(jnp.where(diag, fold(nt(hi_lo(r_rows), wk[...])), 0.0), axis=0, keepdims=True)

    gq_part = jnp.where(iota((SLOT, HDS), 0) == 0, query_grad(r_part), 0.0)
    gp_part = fold(nn(hi_lo(gq_part), wq[...]))
    slot = t * SP + s
    for i in range(WIDTH // TOK):
        gprx[slot, i:i + 1, :] = gp_part[0:1, i * TOK:(i + 1) * TOK]
    gp_copies = [remote(gprx.at[slot], gprx.at[slot], (dp, tps[k], sps[d])) for k in (2, 1, 3, 0) for d in (3, 2, 1, 0) if (k, d) != (0, 0)]

    arrive(pl_copies)
    pool_s[...] = pl_all[...].astype(BF16)
    put(pool_s, pooled_o)
    arrive(ga_copies)
    ga_s[...] = ga_all[...].astype(BF16)
    put(ga_s, ga_o)
    arrive(hbg_copies)
    hb_s[...] = hbg[...].astype(BF16)
    put(hb_s, hb_o)
    arrive(r_copies)
    r_sum = rrx[0] + rrx[1] + rrx[2] + rrx[3]
    small_s[...] = r_sum
    small_s[3:4, :] = jnp.zeros((1, WIDTH), F32)
    small_s[4:5, :] = jnp.zeros((1, WIDTH), F32)
    small_s[3:4, 0:HDS] = query_grad(r_sum)
    small_s[4:5, 0:HDS] = query[0:1]
    arrive(gp_copies)
    gp = sum(gprx[i] for i in range(TP * SP))
    for i in range(WIDTH // TOK):
        small_s[5:6, i * TOK:(i + 1) * TOK] = gp[i:i + 1]
    put(small_s, small_o)
    for copy in started:
        copy.wait_send()
    for copy in puts:
        copy.wait()


N_MESSAGES = 112


def middle(*args):
    vm, sds = pltpu.VMEM, jax.ShapeDtypeStruct
    wide = sds((IMGS, WIDTH), BF16)
    outs = (wide, sds((SLOT, WIDTH), F32), sds((ROWS, WIDTH), BF16), sds((IMGS, 2 * SLOTS, TOK), BF16), sds((IMGS, SLOTS, WIDTH), BF16), sds((SLOTS, WIDTH), BF16), sds((IMGS, TOK), F32),
            wide, wide, wide, wide, sds((IMGS, 256), F32), sds((IMGS, 256), F32), sds((HEADS, IMGS, WIDTH), BF16))
    scratch = [vm((ROWS, WIDTH), BF16)] + [vm((GROUP * TOK, WIDTH), BF16)] * 4 + [vm((WIDTH, WIDTH), BF16), vm((WIDTH, WIDTH), BF16), vm((TP, SLOT, WIDTH), F32),
               *([vm((PAIRS, SLOT, GROUP * TOK), F32)] * 8), vm((TOK, TOK), F32), vm((SP, SP, 2 * SLOTS, TOK), F32), vm((SP, SLOTS, TOK), F32), vm((SP, PAIRS, SLOT, TOK), F32), vm((SP, PAIRS, SLOT, TOK), F32),
               vm((SP, HEADS, GROUP, WIDTH), F32), vm((SP, HEADS, GROUP, WIDTH), F32), vm((HEADS, IMGS, WIDTH), F32),
               vm((TP, GROUP, WIDTH), F32), vm((IMGS, WIDTH), F32), vm((IMGS, 256), F32),
               vm((IMGS, WIDTH), F32), vm((TP, GROUP, WIDTH), F32), vm((TP, GROUP, WIDTH), F32), vm((IMGS, WIDTH), F32),
               vm((IMGS, WIDTH), F32), vm((TP, HDS, WIDTH), F32), vm((TP, IMGS, 256), F32), vm((SP, TP, GROUP * SLOT, HDS), F32), vm((SP, PAIRS, GROUP * SLOT, WIDTH), F32),
               vm((IMGS, 2 * SLOTS, TOK), BF16), vm((IMGS, SLOTS, WIDTH), BF16), vm((SLOTS, WIDTH), BF16), vm((IMGS, TOK), F32),
               vm((IMGS, WIDTH), BF16), vm((IMGS, WIDTH), BF16), vm((IMGS, WIDTH), BF16), vm((IMGS, WIDTH), BF16), vm((HEADS, IMGS, WIDTH), BF16), vm((IMGS, WIDTH), BF16), vm((SLOT, WIDTH), F32), vm((2 * SLOT, WIDTH), F32),
               vm((SP, SLOT, WIDTH), F32), vm((TP * SP, SLOT, TOK), F32),
               pltpu.SemaphoreType.DMA((32,)), pltpu.SemaphoreType.DMA((N_MESSAGES,)), pltpu.SemaphoreType.DMA((N_MESSAGES,))]
    any_spec, vm_spec = pl.BlockSpec(memory_space=pl.ANY), pl.BlockSpec(memory_space=vm)
    in_specs = [any_spec] + [vm_spec] * 14 + [any_spec] * 2 + [vm_spec]
    out_specs = [any_spec] * len(outs)
    return pl.pallas_call(middle_kernel, out_shape=outs, in_specs=in_specs, out_specs=out_specs, scratch_shapes=scratch,
                          compiler_params=pltpu.CompilerParams(collective_id=0, has_side_effects=True, vmem_limit_bytes=63 * 1024 * 1024), name='middle')(*args)


CHUNKS = 16
AHEAD = 5


def final_kernel(xh, a, z, uc, coef, y, gpre, hid, og, o, ga, go, hb, small, probe, pool,
                 gx, gup, gdown, gout, gvalue, gquery, gkey, gprobe, pooled,
                 x_v, gx_v, a_v, z_v, coef_v, uc_v, small_v, pool_v, y_v, gpre_v, hid_v, og_v, o_v, ga_v, go_v, hb_v, gup_v, gdown_v, gout_v, gvalue_v, gquery_v, gkey_v, in_sem, x_sem, az_sem, out_sem, gx_sem):
    images = IMGS // CHUNKS
    rows = images * TOK
    parts = 4

    def block(ref, i, size):
        return ref.at[pl.ds(pl.multiple_of(i * size, size), size)]

    def x_in(i):
        return pltpu.make_async_copy(block(xh, i, rows), block(x_v, i, rows), x_sem.at[i])

    def gx_out(i):
        return pltpu.make_async_copy(block(gx_v, i, rows), block(gx, i, rows), gx_sem.at[i])

    az = [pltpu.make_async_copy(block(src, i, IMGS // parts), block(dst, i, IMGS // parts), az_sem.at[2 * i + n]) for i in range(parts) for n, (src, dst) in enumerate(((a, a_v), (z, z_v)))]
    pairs = ((coef, coef_v), (uc, uc_v), (small, small_v), (pool, pool_v), (y, y_v), (gpre, gpre_v), (hid, hid_v), (og, og_v), (o, o_v), (ga, ga_v), (go, go_v), (hb, hb_v))
    ins = [pltpu.make_async_copy(src, dst, in_sem.at[n]) for n, (src, dst) in enumerate(pairs)]
    for copy in ins[:2] + az[:2]:
        copy.start()
    x_in(0).start()
    x_in(1).start()
    for copy in ins[2:] + az[2:]:
        copy.start()
    for c in range(2, AHEAD):
        x_in(c).start()
    outs = []

    def put(src, dst):
        outs.append(pltpu.make_async_copy(src, dst, out_sem.at[len(outs)]))
        outs[-1].start()

    ins[0].wait()
    ins[1].wait()
    cols = jnp.concatenate([coef_v[...]] * (TOK // IMGS), axis=0).T
    col_lane = iota((TOK, TOK), 1)

    def chunk_step(c):
        x_in(c).wait()
        for j in range(images):
            b = c * images + j
            start = pl.ds(pl.multiple_of(b * TOK, TOK), TOK)
            mixed = tn(a_v[b], jnp.concatenate([uc_v[...], z_v[b]], axis=0))
            col = jnp.sum(jnp.where(col_lane == b, cols, 0.0), axis=1, keepdims=True)
            gx_v[start] = (mixed + x_v[start].astype(F32) * col).astype(BF16)
        gx_out(c).start()

        @pl.when(c + AHEAD < CHUNKS)
        def _():
            x_in(c + AHEAD).start()

    for part in range(parts):
        az[2 * part].wait()
        az[2 * part + 1].wait()
        pl.loop(part * CHUNKS // parts, (part + 1) * CHUNKS // parts)(chunk_step)
        if part == 0:
            for copy in ins[2:]:
                copy.wait()
            turned = jnp.concatenate([small_v[...], jnp.zeros((TOK - SLOT, WIDTH), F32)], axis=0)[:, :256].T
            gquery_v[...] = turned[:HDS, 3:4] * probe[...].reshape(1, WIDTH)
            put(gquery_v, gquery)
            for h in range(HEADS):
                gkey_v[h * HD:(h + 1) * HD] = turned[h * HD:(h + 1) * HD, 4:5] * small_v[h:h + 1]
            put(gkey_v, gkey)
            gprobe[...] = small_v[5]
            put(pool_v, pooled)
            gup_v[...] = tn(y_v[...], gpre_v[...])
            put(gup_v, gup)
        if part == 1:
            gdown_v[...] = tn(hid_v[...], og_v[...])
            put(gdown_v, gdown)
        if part == 2:
            gout_v[...] = tn(o_v[...].astype(BF16), ga_v[...])[:HDS]
            put(gout_v, gout)
            for h in range(HEADS):
                gvalue_v[h * HD:(h + 1) * HD] = tn(go_v[...].astype(BF16), hb_v[h])[h * HD:(h + 1) * HD]
            put(gvalue_v, gvalue)
    for copy in outs:
        copy.wait()

    @pl.loop(0, CHUNKS)
    def _(c):
        gx_out(c).wait()


def final(*args):
    sds, vm = jax.ShapeDtypeStruct, pltpu.VMEM
    outs = (sds((ROWS, WIDTH), BF16), sds((WIDTH, WIDTH), F32), sds((WIDTH, WIDTH), F32)) + (sds((HDS, WIDTH), F32),) * 4 + (sds((WIDTH,), F32), sds((IMGS, WIDTH), BF16))
    any_spec, vm_spec = pl.BlockSpec(memory_space=pl.ANY), pl.BlockSpec(memory_space=vm)
    in_specs = [any_spec] * 14 + [vm_spec, any_spec]
    wide = vm((IMGS, WIDTH), BF16)
    scratch = [vm((ROWS, WIDTH), BF16), vm((ROWS, WIDTH), BF16), vm((IMGS, 2 * SLOTS, TOK), BF16), vm((IMGS, SLOTS, WIDTH), BF16),
               vm((IMGS, TOK), F32), vm((SLOTS, WIDTH), BF16), vm((SLOT, WIDTH), F32), wide, wide, wide, wide, wide, vm((IMGS, 256), F32), wide, vm((IMGS, 256), F32), vm((HEADS, IMGS, WIDTH), BF16),
               vm((WIDTH, WIDTH), F32), vm((WIDTH, WIDTH), F32)] + [vm((HDS, WIDTH), F32)] * 4
    scratch += [pltpu.SemaphoreType.DMA((n,)) for n in (12, CHUNKS, 8, 7, CHUNKS)]
    return pl.pallas_call(final_kernel, out_shape=outs, in_specs=in_specs, out_specs=[any_spec] * 7 + [vm_spec, any_spec], scratch_shapes=scratch,
                          compiler_params=pltpu.CompilerParams(vmem_limit_bytes=63 * 1024 * 1024), name='final')(*args)


def local_head(encoded, enc_gain, enc_bias, probe, w_query, b_query, w_key, w_value, b_value, w_out, b_out, head_gain, head_bias, w_up, b_up, w_down, b_down, out_grad):
    def flat(w):
        return jnp.transpose(w, (1, 2, 0)).reshape(HDS, WIDTH)

    def unflat(g):
        return jnp.transpose(g.reshape(HEADS, HD, WIDTH), (2, 0, 1))

    x = encoded.reshape(ROWS, WIDTH)
    pool, small, xh, a, z, uc, coef, y, hid, gpre, ga, o, go, hb = middle(
        x, enc_gain, enc_bias, probe, flat(w_query), flat(w_key), flat(w_value), w_out.reshape(HDS, WIDTH), b_query, b_value,
        b_out, head_gain, head_bias, b_up, b_down, w_up, w_down, out_grad)
    grad_x, grad_w_up, grad_w_down, grad_w_out, grad_w_value, grad_w_query, grad_w_key, grad_probe, pooled = final(
        xh, a, z, uc, coef, y, gpre, hid, out_grad, o, ga, go, hb, small, probe, pool)
    return (pooled, grad_x.reshape(IMGS, TOK, WIDTH), grad_probe, unflat(grad_w_query), unflat(grad_w_key), unflat(grad_w_value),
            grad_w_out.reshape(HEADS, HD, WIDTH), grad_w_up, grad_w_down)


def solution(mesh):
    return jax.shard_map(local_head, mesh=mesh, in_specs=IN_SPECS, out_specs=OUT_SPECS, check_vma=False)
```
